32 devices in a mesh: gx: 2 (over y), gy: 4 (over x, core), gz: 4 (over z).
Axes of the slice: x: 2, y: 2, z: 4, core: 2. Of those that a mesh axis runs over, the one named last changes fastest.
Arguments:
- features: bfloat16 [6, 8, 32, 8, 128], P('gx', 'gy', 'gz'), may hold values from -6 to 6
- positions: float32 [6, 8, 32, 24], P('gx', 'gy', 'gz'), may hold values from 0 to 256, as said below
- grid_anchor: int32 [6, 8, 32, 24], P('gx', 'gy', 'gz'), may hold values from -1 to 254, as said below
- species: int32 [6, 8, 32, 8], P('gx', 'gy', 'gz'), may hold values from 0 to 1
- neighbours: int32 [6, 8, 32, 512], P('gx', 'gy', 'gz'), may hold values from 0 to 12287, as said below
- neighbour_count: int32 [6, 8, 32, 8], P('gx', 'gy', 'gz'), may hold values from 32 to 64
- w_self: bfloat16 [128, 128], replicated, may hold values from -0.5 to 0.5
- w_neighbour: bfloat16 [128, 128], replicated, may hold values from -0.5 to 0.5
- w_radial: bfloat16 [8, 128], replicated, may hold values from -2 to 2
- radial_rates: float32 [8], replicated, may hold values from 0.05 to 2
- w_pair1: bfloat16 [128, 128], replicated, may hold values from -0.5 to 0.5
- w_pair2: bfloat16 [128, 128], replicated, may hold values from -0.5 to 0.5
- w_vector: bfloat16 [128, 128], replicated, may hold values from -0.5 to 0.5
- w_out: bfloat16 [128, 128], replicated, may hold values from -0.5 to 0.5
- w_charge: bfloat16 [128], replicated, may hold values from -0.5 to 0.5
- species_charge: float32 [2], replicated, may hold values from -1 to 1
Outputs:
- features_out: bfloat16 [6, 8, 32, 8, 128], P('gx', 'gy', 'gz')
- site_potential: float32 [6, 8, 32, 8], P('gx', 'gy', 'gz')
The draws below stay inside these ranges and needn't reach their ends.
Inputs may be any that keep to these rules, and one draw needn't show every extreme that they name: `positions`: component d of slot s of cell (cx, cy, cz) lies in that cell: between c_d * 8 and (c_d + 1) * 8. `grid_anchor`: at the same place as in positions, the whole part of the coordinate minus 1; the coordinate lies between grid_anchor + 1 and grid_anchor + 2. `neighbours`: each entry is the index ((cx * 8 + cy) * 32 + cz) * 8 + s of an atom whose cell differs from the listing atom's cell by at most one along each dimension, periodically; never the listing atom itself.
All inputs are finite; a program needn't handle non-finite values.
Results may differ from the reference program's by a relative error of at most 0.0039.
The reference program's roundings to bfloat16 on the way count: a program that leaves them out, or rounds other values in their place, can miss the bound.
Values may be sent and summed in bfloat16 or wider, within the bound.
A program may use at most 64 MiB of HBM per device.

```python
import math
import jax
import jax.numpy as jnp
from jax import lax

C = 128
K = 8
NBR = 64
SPECIES = 2
CELL = 8
BLOCK = 128
SLOTS = 8
NCX = 6
NCY = 8
NCZ = 32
NX = 48
NY = 64
NZ = 256
SCREEN = 32


def cell_corners():
    cell_x = jnp.broadcast_to(jnp.arange(NCX, dtype=jnp.int32)[:, None, None], (NCX, NCY, NCZ))
    cell_y = jnp.broadcast_to(jnp.arange(NCY, dtype=jnp.int32)[None, :, None], (NCX, NCY, NCZ))
    cell_z = jnp.broadcast_to(jnp.arange(NCZ, dtype=jnp.int32)[None, None, :], (NCX, NCY, NCZ))
    return (jnp.stack([cell_x, cell_y, cell_z], axis=3) * CELL)[:, :, :, :, None]


def placement_parts(key):
    inner_cell = jax.random.randint(jax.random.fold_in(key, 11), (NCX, NCY, NCZ, 3, SLOTS), 0, CELL)
    return cell_corners() + inner_cell


def draw_positions(key, part):
    whole_cells = placement_parts(key)
    uniform_draw = jax.random.uniform(jax.random.fold_in(key, 12), (NCX, NCY, NCZ, 3, SLOTS), jnp.float32)
    fraction = uniform_draw
    return (whole_cells.astype(jnp.float32) + fraction).reshape(NCX, NCY, NCZ, 3 * SLOTS)


def draw_grid_anchor(key, part):
    return (placement_parts(key) - 1).reshape(NCX, NCY, NCZ, 3 * SLOTS).astype(jnp.int32)


def draw_neighbours(key, part):
    draw_shape = (NCX, NCY, NCZ, SLOTS, NBR)
    steps_x = jax.random.randint(jax.random.fold_in(key, 21), draw_shape, -1, 2)
    steps_y = jax.random.randint(jax.random.fold_in(key, 22), draw_shape, -1, 2)
    steps_z = jax.random.randint(jax.random.fold_in(key, 23), draw_shape, -1, 2)
    pick_slot = jax.random.randint(jax.random.fold_in(key, 24), draw_shape, 0, SLOTS)
    cell_x = jnp.arange(NCX, dtype=jnp.int32)[:, None, None, None, None]
    cell_y = jnp.arange(NCY, dtype=jnp.int32)[None, :, None, None, None]
    cell_z = jnp.arange(NCZ, dtype=jnp.int32)[None, None, :, None, None]
    own_slot = jnp.arange(SLOTS, dtype=jnp.int32)[None, None, None, :, None]
    self_pair = (steps_x == 0) & (steps_y == 0) & (steps_z == 0) & (pick_slot == own_slot)
    pick_slot = jnp.where(self_pair, (pick_slot + 1) % SLOTS, pick_slot)
    other_x = (cell_x + steps_x) % NCX
    other_y = (cell_y + steps_y) % NCY
    other_z = (cell_z + steps_z) % NCZ
    atom_ids = ((other_x * NCY + other_y) * NCZ + other_z) * SLOTS + pick_slot
    return atom_ids.reshape(NCX, NCY, NCZ, SLOTS * NBR).astype(jnp.int32)


def with_ends(entries, own_key, smallest, high):
    shape = entries.shape
    spot = [jax.random.randint(jax.random.fold_in(own_key, axis), (), 0, shape[axis]) for axis in range(len(shape))]
    entries = entries.at[tuple(spot)].set(smallest)
    longest = shape.index(max(shape))
    spot[longest] = (spot[longest] + 1) % shape[longest]
    return entries.at[tuple(spot)].set(high)


def levels(key, shape, shards, low, largest):
    level, own = 1.0, jax.random.fold_in(key, 6)
    for axis_at, blocks in shards:
        heights = jnp.exp(jax.random.uniform(jax.random.fold_in(own, axis_at), (blocks,), jnp.float32, low / len(shards), largest / len(shards)))
        level = level * jnp.repeat(heights, shape[axis_at] // blocks).reshape([-1 if axis == axis_at else 1 for axis in range(len(shape))])
    return level


def noise(rng, shape, scale, most, pieces=(), kind=jnp.bfloat16):
    entries = scale * jax.random.normal(rng, shape, jnp.float32)
    if pieces:
        entries = entries * levels(rng, shape, pieces, -0.22, 0.18)
    return jnp.clip(entries, -most, most).astype(kind)


def setup_inputs(seed: int = 0) -> dict:
    key_of = jax.random.split(jax.random.key(seed), 17)
    return {
        "features": noise(key_of[0], (NCX, NCY, NCZ, SLOTS, C), 1.0, 6.0, ((0, 2), (1, 4), (2, 4))),
        "positions": draw_positions(jax.random.fold_in(key_of[16], 71), 0),
        "grid_anchor": draw_grid_anchor(jax.random.fold_in(key_of[16], 71), 0),
        "species": with_ends(jax.random.randint(key_of[3], (NCX, NCY, NCZ, SLOTS), 0, SPECIES), jax.random.fold_in(key_of[3], 1), 0, SPECIES - 1).astype(jnp.int32),
        "neighbours": draw_neighbours(jax.random.fold_in(key_of[16], 71), 0),
        "neighbour_count": with_ends(jax.random.randint(key_of[5], (NCX, NCY, NCZ, SLOTS), NBR // 2, NBR + 1), jax.random.fold_in(key_of[5], 1), NBR // 2, NBR).astype(jnp.int32),
        "w_self": noise(key_of[6], (C, C), C ** -0.5, 0.5),
        "w_neighbour": noise(key_of[7], (C, C), C ** -0.5, 0.5),
        "w_radial": noise(key_of[8], (K, C), K ** -0.5, 2.0),
        "radial_rates": jnp.clip(jnp.exp(jax.random.uniform(key_of[9], (K,), jnp.float32, math.log(0.05), math.log(2.0))), 0.05, 2.0),
        "w_pair1": noise(key_of[10], (C, C), C ** -0.5, 0.5),
        "w_pair2": noise(key_of[11], (C, C), C ** -0.5, 0.5),
        "w_vector": noise(key_of[12], (C, C), C ** -0.5, 0.5),
        "w_out": noise(key_of[13], (C, C), C ** -0.5, 0.5),
        "w_charge": noise(key_of[14], (C,), C ** -0.5, 0.5),
        "species_charge": jnp.clip(jax.random.uniform(key_of[15], (SPECIES,), jnp.float32, -1.0, 1.0), -1.0, 1.0),
    }


coulomb_scale = 0.25
smearing = 1.0
highest = lax.Precision.HIGHEST

def spline_weights(fraction):
    square = fraction * fraction
    cube_part = square * fraction
    remain = 1.0 - fraction
    return jnp.stack([remain * remain * remain / 6.0, (3.0 * cube_part - 6.0 * square + 4.0) / 6.0, (-3.0 * cube_part + 3.0 * square + 3.0 * fraction + 1.0) / 6.0, cube_part / 6.0], axis=-1)

def wave_squared(mode_ids, length):
    signed_modes = jnp.where(mode_ids > length // 2, mode_ids - length, mode_ids).astype(jnp.float32)
    wavenumber = signed_modes * (2.0 * math.pi / length)
    return wavenumber * wavenumber

def spline_modulus(mode_ids, length):
    real_part = jnp.zeros(mode_ids.shape, jnp.float32)
    imag_part = jnp.zeros(mode_ids.shape, jnp.float32)
    for tap_shift, coefficient in ((0, 1.0 / 6.0), (1, 4.0 / 6.0), (2, 1.0 / 6.0)):
        angles = (mode_ids * tap_shift % length).astype(jnp.float32) * (2.0 * math.pi / length)
        real_part = real_part + coefficient * jnp.cos(angles)
        imag_part = imag_part + coefficient * jnp.sin(angles)
    return real_part * real_part + imag_part * imag_part

def green_values(mode_x, mode_y, mode_z, length_x, length_y, length_z, screen_length):
    total_sq = wave_squared(mode_x, length_x) + wave_squared(mode_y, length_y) + wave_squared(mode_z, length_z)
    moduli = spline_modulus(mode_x, length_x) * spline_modulus(mode_y, length_y) * spline_modulus(mode_z, length_z)
    kernel = coulomb_scale * 4.0 * math.pi * jnp.exp(-0.5 * smearing * smearing * total_sq) / ((total_sq + 1.0 / (screen_length * screen_length)) * moduli)
    zero_mode = (mode_x == 0) & (mode_y == 0) & (mode_z == 0)
    return jnp.where(zero_mode, 0.0, kernel)

def atom_table(values):
    cell_shape = values.shape[:3]
    slot_count = values.shape[3] // 3
    grouped = values.reshape(cell_shape + (3, slot_count))
    return jnp.moveaxis(grouped, 3, 4).reshape(-1, 3)

def atom_update(hidden_rows, own_proj, sent_rows, displace, live_slots, w_radial, radial_rates, w_pair1, w_pair2, w_vector, w_out):
    row_count, list_length, channels = sent_rows.shape
    scaled = displace / CELL
    square = lax.optimization_barrier(jnp.sum(scaled * scaled, axis=2))
    radial_basis = jnp.exp(-square[:, :, None] * radial_rates[None, None, :]).astype(jnp.bfloat16)
    radial_part = jnp.dot(radial_basis.reshape(row_count * list_length, -1), w_radial, preferred_element_type=jnp.float32)
    pre_active = own_proj[:, None, :] + sent_rows.astype(jnp.float32) + radial_part.reshape(row_count, list_length, channels)
    latent = jax.nn.silu(pre_active).astype(jnp.bfloat16).reshape(row_count * list_length, channels)
    second = jax.nn.silu(jnp.dot(latent, w_pair1, preferred_element_type=jnp.float32)).astype(jnp.bfloat16)
    third_layer = jax.nn.silu(jnp.dot(second, w_pair2, preferred_element_type=jnp.float32)).astype(jnp.bfloat16)
    vector_weights = jnp.dot(third_layer, w_vector, preferred_element_type=jnp.float32).reshape(row_count, list_length, channels)
    live_float = live_slots.astype(jnp.float32)
    message = jnp.einsum('rn,rnc->rc', live_float, third_layer.reshape(row_count, list_length, channels).astype(jnp.float32), precision=highest) / NBR
    weighted = live_float[:, :, None] * scaled
    vector = jnp.einsum('rnd,rnc->rdc', weighted, vector_weights, precision=highest) / math.sqrt(NBR)
    invariant = lax.optimization_barrier(jnp.sum(vector * vector, axis=1))
    update = (message + invariant).astype(jnp.bfloat16)
    return (hidden_rows.astype(jnp.float32) + jnp.dot(update, w_out, preferred_element_type=jnp.float32)).astype(jnp.bfloat16)

def reference(features, positions, grid_anchor, species, neighbours, neighbour_count, w_self, w_neighbour, w_radial, radial_rates, w_pair1, w_pair2, w_vector, w_out, w_charge, species_charge):
    atom_count = NCX * NCY * NCZ * SLOTS
    hidden_rows = features.reshape(atom_count, C)
    place_rows = atom_table(positions)
    anchor_rows = atom_table(grid_anchor)
    species_rows = species.reshape(atom_count)
    neighbour_rows = neighbours.reshape(atom_count, NBR)
    counts = neighbour_count.reshape(atom_count)
    own_proj = jnp.dot(hidden_rows, w_self, preferred_element_type=jnp.float32)
    sent_proj = jnp.dot(hidden_rows, w_neighbour, preferred_element_type=jnp.float32).astype(jnp.bfloat16)
    box_length = jnp.array([NCX * CELL, NCY * CELL, NCZ * CELL], jnp.float32)
    list_ids = jnp.arange(NBR, dtype=jnp.int32)

    def pair_block(block_index):
        block_start = (block_index * BLOCK).astype(jnp.int32)
        block_ids = lax.dynamic_slice_in_dim(neighbour_rows, block_start, BLOCK, 0)
        own_place = lax.dynamic_slice_in_dim(place_rows, block_start, BLOCK, 0)
        displace = place_rows[block_ids] - own_place[:, None, :]
        displace = displace - box_length * jnp.floor(displace / box_length + 0.5)
        live_slots = list_ids[None, :] < lax.dynamic_slice_in_dim(counts, block_start, BLOCK, 0)[:, None]
        return atom_update(lax.dynamic_slice_in_dim(hidden_rows, block_start, BLOCK, 0), lax.dynamic_slice_in_dim(own_proj, block_start, BLOCK, 0), sent_proj[block_ids], displace, live_slots, w_radial, radial_rates, w_pair1, w_pair2, w_vector, w_out)
    updated = lax.map(pair_block, jnp.arange(atom_count // BLOCK, dtype=jnp.int32))
    features_out = updated.reshape(NCX, NCY, NCZ, SLOTS, C)
    charge = species_charge[species_rows] + jnp.dot(hidden_rows, w_charge, preferred_element_type=jnp.float32)
    tap_weights = spline_weights(place_rows - (anchor_rows + 1).astype(jnp.float32))
    tap_ids = jnp.arange(4, dtype=jnp.int32)
    index_x = (anchor_rows[:, 0:1] + tap_ids[None, :]) % NX
    index_y = (anchor_rows[:, 1:2] + tap_ids[None, :]) % NY
    index_z = (anchor_rows[:, 2:3] + tap_ids[None, :]) % NZ
    stencil = tap_weights[:, 0, :, None, None] * tap_weights[:, 1, None, :, None] * tap_weights[:, 2, None, None, :]
    amounts = charge[:, None, None, None] * stencil
    charge_grid = jnp.zeros((NX, NY, NZ), jnp.float32).at[index_x[:, :, None, None], index_y[:, None, :, None], index_z[:, None, None, :]].add(amounts)
    spectrum = jnp.fft.fftn(charge_grid)
    green = green_values(jnp.arange(NX, dtype=jnp.int32)[:, None, None], jnp.arange(NY, dtype=jnp.int32)[None, :, None], jnp.arange(NZ, dtype=jnp.int32)[None, None, :], NX, NY, NZ, SCREEN)
    potential_grid = jnp.real(jnp.fft.ifftn(spectrum * green)).astype(jnp.float32)
    sampled = potential_grid[index_x[:, :, None, None], index_y[:, None, :, None], index_z[:, None, None, :]]
    site_potential = lax.optimization_barrier(jnp.sum(sampled * stencil, axis=(1, 2, 3))).reshape(NCX, NCY, NCZ, SLOTS)
    return (features_out, site_potential)
```

```python
import functools
import math

import jax
import jax.numpy as jnp
import numpy as np
from jax import lax
from jax.experimental import pallas as pl
from jax.experimental.pallas import tpu as pltpu
from jax.sharding import PartitionSpec as P

NBR = 64
CELL = 8
AXES = ("gx", "gy", "gz")

coulomb_scale = 0.25
smearing = 1.0
highest = lax.Precision.HIGHEST


def padded(block, sides):
    for axis, dim in sides:
        count = lax.axis_size(axis)
        forward = [(i, (i + 1) % count) for i in range(count)]
        backward = [(target, source) for source, target in forward]
        low = lax.ppermute(
            lax.slice_in_dim(block, block.shape[dim] - 1, None, axis=dim), axis, forward
        )
        high = lax.ppermute(lax.slice_in_dim(block, 0, 1, axis=dim), axis, backward)
        block = jnp.concatenate([low, block, high], axis=dim)
    return block


def round_bf16(x):
    return lax.reduce_precision(x, 8, 7)


def three_pieces(x):
    hi = round_bf16(x)
    mid = round_bf16(x - hi)
    lo = round_bf16(x - hi - mid)
    return hi, mid, lo


def cast_pieces(x, count):
    pieces = []
    for _ in range(count):
        piece = x.astype(jnp.bfloat16)
        pieces.append(piece)
        x = x - piece.astype(jnp.float32)
    return pieces


def silu(v):
    half = 0.5 * v
    return half + half * jnp.tanh(half)


def pair_kernel(
    cells,
    lengths,
    code_ref,
    ext_ref,
    own_ref,
    hidden_ref,
    wr_ref,
    rates_ref,
    w1_ref,
    w2_ref,
    wv_ref,
    wo_ref,
    out_ref,
    msg_ref,
    vec_ref,
    w1t_ref,
    w2t_ref,
):
    cells_x, cells_y, cells_z = cells
    f32, bf16 = jnp.float32, jnp.bfloat16
    slots = 8
    pairs = slots * NBR
    w1t_ref[...] = w1_ref[...].astype(f32).T.astype(bf16)
    w2t_ref[...] = w2_ref[...].astype(f32).T.astype(bf16)
    wr_rows = jnp.concatenate([wr_ref[...].astype(f32), jnp.zeros((8, 128), f32)], axis=1)
    zero_half = jnp.zeros((8, 128), f32)
    lane_slot = lax.broadcasted_iota(jnp.int32, (slots, pairs), 1) // NBR
    sel = jnp.where(lane_slot == lax.broadcasted_iota(jnp.int32, (slots, pairs), 0), 1.0, 0.0)
    tail = jnp.concatenate([sel, sel, sel, jnp.zeros((8, pairs), f32)], axis=0).astype(bf16)
    row_d = lax.broadcasted_iota(jnp.int32, (8, 1), 0)
    box = jnp.where(
        row_d == 0,
        float(lengths[0]),
        jnp.where(row_d == 1, float(lengths[1]), float(lengths[2])),
    )
    box_inv = 1.0 / box
    rates = rates_ref[...]

    def one_cell(c, carry):
        cz = c % cells_z
        cxy = c // cells_z
        cy = cxy % cells_y
        cx = cxy // cells_y
        row = pl.multiple_of(cz * 8, 8)
        here = pl.multiple_of(c * 8, 8)
        parts = []
        for dx in range(3):
            for dy in range(3):
                column = (cx + dx) * (cells_y + 2) + cy + dy
                parts.append(ext_ref[column, pl.ds(row, 24), :])
        mine = ext_ref[(cx + 1) * (cells_y + 2) + cy + 1, pl.ds(row + 8, 8), 128:]
        own = own_ref[pl.ds(here, 8), :]
        own_hi, own_mid, own_lo = [p.astype(f32) for p in cast_pieces(own, 3)]
        parts.append(wr_rows)
        parts.append(jnp.concatenate([own_hi, -mine], axis=1))
        parts.append(jnp.concatenate([own_mid, zero_half], axis=1))
        parts.append(jnp.concatenate([own_lo, zero_half], axis=1))
        parts.append(jnp.zeros((8, 256), f32))
        table = jnp.concatenate(parts, axis=0)
        sent_t = table[:, :128].T.astype(bf16)
        place_t = table[:, 128:].T[:32].astype(bf16)
        code = code_ref[c]
        which = code & 255
        live = jnp.where(code < 256, 1.0, 0.0)
        hot = jnp.where(
            lax.broadcasted_iota(jnp.int32, (216, pairs), 0) == which, 1.0, 0.0
        )
        hot_main = hot[:208].astype(bf16)
        hot_last = hot[208:]
        rhs_place = jnp.concatenate(
            [
                hot_main,
                jnp.concatenate([hot_last, jnp.zeros((8, pairs), f32)], axis=0).astype(bf16),
                tail,
            ],
            axis=0,
        )
        found = jnp.dot(place_t, rhs_place, preferred_element_type=f32)
        displace = found[0:8] + found[8:16] + found[16:24]
        displace = displace - box * jnp.floor(displace * box_inv + 0.5)
        scaled = displace * (1.0 / CELL)
        square = jnp.sum(scaled * scaled, axis=0, keepdims=True)
        basis = jnp.exp(-square * rates)
        rhs = jnp.concatenate(
            [hot_main, jnp.concatenate([hot_last, basis], axis=0).astype(bf16), tail], axis=0
        )
        pre = jnp.dot(sent_t, rhs, preferred_element_type=f32)
        latent = silu(pre).astype(bf16)
        second = silu(jnp.dot(w1t_ref[...], latent, preferred_element_type=f32)).astype(bf16)
        third = silu(jnp.dot(w2t_ref[...], second, preferred_element_type=f32)).astype(bf16)
        reach = scaled * live
        pieces = [p.astype(f32) for p in cast_pieces(reach, 3)]
        rows = [sel * live]
        for d in range(3):
            for piece in pieces:
                rows.append(sel * piece[d : d + 1])
        weights = jnp.concatenate(rows, axis=0).astype(bf16)
        sums = lax.dot_general(
            weights, third, (((1,), (1,)), ((), ())), preferred_element_type=f32
        )
        msg_ref[pl.ds(here, 8), :] = sums[0:8] * (1.0 / NBR)
        for d in range(3):
            base = 8 + 24 * d
            vec_ref[d, pl.ds(here, 8), :] = (
                sums[base : base + 8] + sums[base + 8 : base + 16] + sums[base + 16 : base + 24]
            )
        return carry

    lax.fori_loop(0, cells_x * cells_y * cells_z, one_cell, 0)
    wv = wv_ref[...].astype(f32)
    invariant = None
    for d in range(3):
        vector = jnp.dot(
            vec_ref[d], wv, precision=highest, preferred_element_type=f32
        ) * (1.0 / math.sqrt(NBR))
        part = vector * vector
        invariant = part if invariant is None else invariant + part
    update = (msg_ref[...] + invariant).astype(bf16)
    out_ref[...] = (
        hidden_ref[...].astype(f32)
        + jnp.dot(update, wo_ref[...], preferred_element_type=f32)
    ).astype(bf16)


def spline(distance):
    outer = jnp.maximum(2.0 - distance, 0.0)
    inner = jnp.maximum(1.0 - distance, 0.0)
    return (outer * outer * outer - 4.0 * (inner * inner * inner)) * (1.0 / 6.0)


def trig_basis(length):
    r = np.arange(length)
    rows = [np.cos(2 * np.pi * ((k * r) % length) / length) for k in range(length // 2 + 1)]
    rows += [np.sin(2 * np.pi * ((k * r) % length) / length) for k in range(1, length // 2)]
    modes = np.array(list(range(length // 2 + 1)) + list(range(1, length // 2)))
    return np.stack(rows), modes


def axis_terms(modes, length):
    wave = modes * (2.0 * np.pi / length)
    turn = np.exp(2j * np.pi * modes / length)
    modulus = np.abs(1 / 6 + 4 / 6 * turn + 1 / 6 * turn * turn) ** 2
    weight = np.where((modes == 0) | (2 * modes == length), 1.0, 2.0) / length
    return wave * wave, weight / modulus


def charge_kernel(
    sizes,
    lengths,
    window,
    screen,
    planes,
    atoms_ref,
    zrow_ref,
    krow_ref,
    kx_ref,
    by_ref,
    byt_ref,
    bx_ref,
    bxt_ref,
    out_ref,
    plane_ref,
    wave_ref,
):
    devices_x, devices_y, devices_z = sizes
    length_x, length_y, length_z = lengths
    grid_y = length_y // devices_y
    f32, bf16 = jnp.float32, jnp.bfloat16
    lanes = atoms_ref.shape[-1] * devices_z

    def load(gx, gy):
        base = (gx * devices_y + gy) * devices_z
        return jnp.concatenate([atoms_ref[base + i] for i in range(devices_z)], axis=1)

    def stencils(atoms, gy):
        ids_x = lax.broadcasted_iota(jnp.int32, (length_x, lanes), 0).astype(f32)
        off_x = jnp.abs(ids_x - atoms[0:1])
        rows_x = spline(jnp.minimum(off_x, length_x - off_x))
        start = (gy * grid_y - 1).astype(f32)
        ids_y = lax.broadcasted_iota(jnp.int32, (window, lanes), 0).astype(f32)
        rows_y = spline(jnp.abs(ids_y - (atoms[1:2] - start)))
        return rows_x, rows_y

    zrow = zrow_ref[...]

    def spread(gx, gy):
        atoms = load(gx, gy)
        rows_x, rows_y = stencils(atoms, gy)
        place_z = atoms[2:3]
        whole = jnp.floor(place_z)
        f = place_z - whole
        sq = f * f
        cube = sq * f
        rem = 1.0 - f
        taps = [
            rem * rem * rem * (1.0 / 6.0),
            (3.0 * cube - 6.0 * sq + 4.0) * (1.0 / 6.0),
            (-3.0 * cube + 3.0 * sq + 3.0 * f + 1.0) * (1.0 / 6.0),
            cube * (1.0 / 6.0),
        ]
        turns = zrow[:, 0:1] * (whole - 1.0)
        turns = turns - length_z * jnp.floor(turns * (1.0 / length_z))
        angle = (turns - 0.5 * length_z) * (2.0 * math.pi / length_z)
        cos_a = -jnp.cos(angle)
        sin_a = -jnp.sin(angle)
        shift_c = zrow[:, 1:2]
        shift_s = zrow[:, 2:3]
        base_c = cos_a * shift_c + sin_a * shift_s
        base_s = sin_a * shift_c - cos_a * shift_s
        even = taps[0]
        odd = 0.0
        for t in range(1, 4):
            even = even + taps[t] * zrow[:, 2 + t : 3 + t]
            odd = odd + taps[t] * zrow[:, 5 + t : 6 + t]
        wave = base_c * even - base_s * odd
        wave_ref[gx * devices_y + gy] = wave
        scaled = wave * atoms[3:4]
        left = jnp.concatenate([rows_y * scaled[j : j + 1] for j in range(planes)], axis=0)
        left_hi = left.astype(bf16)
        left_lo = (left - left_hi.astype(f32)).astype(bf16)
        x_hi = rows_x.astype(bf16)
        x_lo = (rows_x - x_hi.astype(f32)).astype(bf16)
        res = lax.dot_general(
            jnp.concatenate([left_hi, left_lo], axis=0),
            jnp.concatenate([x_hi, x_lo], axis=0),
            (((1,), (1,)), ((), ())),
            preferred_element_type=f32,
        )
        half = planes * window
        res = res[:half] + res[half:]
        return res[:, :length_x] + res[:, length_x:]

    for gy in range(devices_y):
        gy_id = jnp.int32(gy)
        total = lax.fori_loop(
            0,
            devices_x,
            lambda gx, acc: acc + spread(gx, gy_id),
            jnp.zeros((planes * window, length_x), f32),
        )
        for j in range(planes):
            plane_ref[j, gy * window : (gy + 1) * window, :] = total[
                j * window : (j + 1) * window
            ]

    def hdot(a, b):
        return jnp.dot(a, b, precision=highest, preferred_element_type=f32)

    along_y = jnp.concatenate([hdot(by_ref[...], plane_ref[j]) for j in range(planes)], axis=0)
    spectrum = hdot(along_y, bxt_ref[...])
    krow = krow_ref[...]
    q = krow[:, 0:1] + kx_ref[0:1, :]
    scale = krow[:, 1:2] * kx_ref[1:2, :]
    green = (coulomb_scale * 4.0 * math.pi) * jnp.exp(-0.5 * smearing * smearing * q)
    green = green * scale / (q + 1.0 / (screen * screen))
    green = jnp.where(q == 0.0, 0.0, green)
    back = hdot(spectrum * green, bx_ref[...])
    for j in range(planes):
        plane_ref[j] = hdot(byt_ref[...], back[j * length_y : (j + 1) * length_y])

    for gy in range(devices_y):
        gy_id = jnp.int32(gy)
        field = jnp.concatenate(
            [plane_ref[j, gy * window : (gy + 1) * window, :] for j in range(planes)], axis=0
        )
        f_hi, f_mid = [p.astype(f32) for p in cast_pieces(field, 2)]
        field3 = jnp.concatenate([f_hi, f_mid, f_hi], axis=1).astype(bf16)

        def sample(gx, carry):
            atoms = load(gx, gy_id)
            rows_x, rows_y = stencils(atoms, gy_id)
            x_hi = rows_x.astype(bf16)
            x_lo = (rows_x - x_hi.astype(f32)).astype(bf16)
            values = jnp.dot(
                field3,
                jnp.concatenate([x_hi, x_hi, x_lo], axis=0),
                preferred_element_type=f32,
            )
            wave = wave_ref[gx * devices_y + gy_id]
            mixed = values[0:window] * wave[0:1]
            for j in range(1, planes):
                mixed = mixed + values[j * window : (j + 1) * window] * wave[j : j + 1]
            out_ref[gx * devices_y + gy_id] = jnp.sum(mixed * rows_y, axis=0, keepdims=True)
            return carry

        lax.fori_loop(0, devices_x, sample, 0)


def shards(
    features,
    positions,
    grid_anchor,
    species,
    neighbours,
    neighbour_count,
    w_self,
    w_neighbour,
    w_radial,
    radial_rates,
    w_pair1,
    w_pair2,
    w_vector,
    w_out,
    w_charge,
    species_charge,
):
    f32, bf16 = jnp.float32, jnp.bfloat16
    cells_x, cells_y, cells_z, slot_count, channels = features.shape
    cell_count = cells_x * cells_y * cells_z
    atom_count = cell_count * slot_count
    sizes = tuple(lax.axis_size(a) for a in AXES)
    devices = sizes[0] * sizes[1] * sizes[2]
    totals = (cells_x * sizes[0], cells_y * sizes[1], cells_z * sizes[2])
    lengths = tuple(t * CELL for t in totals)
    length_x, length_y, length_z = lengths
    screen = 2 * cells_y * CELL

    hidden = features.reshape(atom_count, channels)
    own = jnp.dot(hidden, w_self, preferred_element_type=f32)
    sent = jnp.dot(hidden, w_neighbour, preferred_element_type=f32).astype(bf16)
    species_rows = species.reshape(atom_count)
    kind_ids = jnp.arange(species_charge.shape[0], dtype=jnp.int32)
    base_charge = jnp.sum(
        jnp.where(species_rows[:, None] == kind_ids[None, :], species_charge[None, :], 0.0), axis=1
    )
    charge = base_charge + jnp.dot(hidden, w_charge, preferred_element_type=f32)
    place = positions.reshape(cell_count, 3, slot_count)
    place_cols = jnp.moveaxis(place, 1, 0).reshape(3, atom_count)
    atoms = jnp.concatenate([place_cols, charge[None]], axis=0)
    atoms = lax.all_gather(atoms, AXES)

    hi, mid, lo = three_pieces(jnp.moveaxis(place, 1, 2).reshape(atom_count, 3))
    gap = jnp.zeros((atom_count, 5), f32)
    place_rows = jnp.concatenate(
        [hi, gap, mid, gap, lo, gap, jnp.zeros((atom_count, channels - 24), f32)], axis=1
    ).astype(bf16)
    rows = jnp.concatenate([sent, place_rows], axis=1)
    rows = rows.reshape(cells_x, cells_y, cells_z, slot_count, 2 * channels)
    ext = padded(rows, (("gx", 0), ("gy", 1), ("gz", 2)))
    ext = ext.astype(f32).reshape(
        (cells_x + 2) * (cells_y + 2), (cells_z + 2) * slot_count, 2 * channels
    )

    listed = neighbours.reshape(cells_x, cells_y, cells_z, slot_count * NBR)
    slot_ids = listed % slot_count
    cell_ids = listed // slot_count
    steps = []
    for axis, ids in enumerate(
        (cell_ids // (totals[2] * totals[1]), cell_ids // totals[2] % totals[1], cell_ids % totals[2])
    ):
        local = lax.broadcasted_iota(jnp.int32, listed.shape, axis)
        first = lax.axis_index(AXES[axis]) * (cells_x, cells_y, cells_z)[axis]
        steps.append((ids - first - local + 1 + totals[axis]) % totals[axis])
    code = ((steps[0] * 3 + steps[1]) * 3 + steps[2]) * slot_count + slot_ids
    counts = neighbour_count.reshape(cell_count, slot_count, 1)
    dead = jnp.arange(NBR, dtype=jnp.int32)[None, None, :] >= counts
    code = code.reshape(cell_count, slot_count, NBR) + jnp.where(dead, 256, 0)
    code = code.reshape(cell_count, 1, slot_count * NBR)

    vmem = pl.BlockSpec(memory_space=pltpu.VMEM)
    updated = pl.pallas_call(
        functools.partial(pair_kernel, (cells_x, cells_y, cells_z), lengths),
        out_shape=jax.ShapeDtypeStruct((atom_count, channels), bf16),
        in_specs=[vmem] * 10,
        out_specs=vmem,
        scratch_shapes=[
            pltpu.VMEM((atom_count, channels), f32),
            pltpu.VMEM((3, atom_count, channels), f32),
            pltpu.VMEM((channels, channels), bf16),
            pltpu.VMEM((channels, channels), bf16),
        ],
        name="pair_layer",
        cost_estimate=pl.CostEstimate(
            flops=2 * atom_count * NBR * channels * 512,
            bytes_accessed=4 * 1024 * 1024,
            transcendentals=3 * atom_count * NBR * channels,
        ),
    )(
        code,
        ext,
        own,
        hidden,
        w_radial,
        radial_rates.reshape(-1, 1),
        w_pair1,
        w_pair2,
        w_vector,
        w_out,
    )

    share = length_z // 2 // devices
    planes = 2 * share
    window = -(-(cells_y * CELL + 4) // 8) * 8
    all_modes = np.arange(length_z // 2)
    table_k = np.stack([all_modes, all_modes], axis=1)
    phase_c = np.stack([np.ones_like(all_modes), np.zeros_like(all_modes)], axis=1)
    table_k[0, 1] = length_z // 2
    phase_c[0, 1] = 1
    table_k = table_k.reshape(devices, planes)
    phase_c = phase_c.reshape(devices, planes).astype(np.float64)
    taps = [2 * np.pi * ((table_k * t) % length_z) / length_z for t in range(1, 4)]
    zrow = np.stack(
        [table_k, phase_c, 1.0 - phase_c]
        + [np.cos(a) for a in taps]
        + [np.sin(a) for a in taps],
        axis=2,
    ).astype(np.float32)
    basis_x, modes_x = trig_basis(length_x)
    basis_y, modes_y = trig_basis(length_y)
    qx, sx = axis_terms(modes_x, length_x)
    qy, sy = axis_terms(modes_y, length_y)
    qz, sz = axis_terms(table_k, length_z)
    krow = np.stack(
        [qz[:, :, None] + qy[None, None, :], sz[:, :, None] * sy[None, None, :]], axis=-1
    )
    krow = krow.reshape(devices, planes * length_y, 2).astype(np.float32)
    kx = np.stack([qx, sx]).astype(np.float32)
    grid_y = cells_y * CELL
    columns = np.concatenate(
        [(np.arange(window) + g * grid_y - 1) % length_y for g in range(sizes[1])]
    )
    by = basis_y[:, columns].astype(np.float32)
    bx = basis_x.astype(np.float32)
    me = lax.axis_index(AXES)
    partial = pl.pallas_call(
        functools.partial(charge_kernel, sizes, lengths, window, screen, planes),
        out_shape=jax.ShapeDtypeStruct((sizes[0] * sizes[1], 1, sizes[2] * atom_count), f32),
        in_specs=[vmem] * 8,
        out_specs=vmem,
        scratch_shapes=[
            pltpu.VMEM((planes, sizes[1] * window, length_x), f32),
            pltpu.VMEM((sizes[0] * sizes[1], planes, sizes[2] * atom_count), f32),
        ],
        name="charge_solve",
        cost_estimate=pl.CostEstimate(
            flops=10**10, bytes_accessed=2 * 1024 * 1024, transcendentals=10**6
        ),
    )(
        atoms,
        lax.dynamic_index_in_dim(jnp.asarray(zrow), me, 0, False),
        lax.dynamic_index_in_dim(jnp.asarray(krow), me, 0, False),
        jnp.asarray(kx),
        jnp.asarray(by),
        jnp.asarray(np.ascontiguousarray(by.T)),
        jnp.asarray(bx),
        jnp.asarray(np.ascontiguousarray(bx.T)),
    )
    site_potential = lax.psum_scatter(
        partial.reshape(devices, atom_count), AXES, scatter_dimension=0, tiled=False
    )
    return (
        updated.reshape(features.shape),
        site_potential.reshape(cells_x, cells_y, cells_z, slot_count),
    )


def solution(mesh):
    return jax.shard_map(
        shards,
        mesh=mesh,
        in_specs=(
            P("gx", "gy", "gz", None, None),
            P("gx", "gy", "gz", None),
            P("gx", "gy", "gz", None),
            P("gx", "gy", "gz", None),
            P("gx", "gy", "gz", None),
            P("gx", "gy", "gz", None),
            P(),
            P(),
            P(),
            P(),
            P(),
            P(),
            P(),
            P(),
            P(),
            P(),
        ),
        out_specs=(P("gx", "gy", "gz", None, None), P("gx", "gy", "gz", None)),
        check_vma=False,
    )
```

```python
import functools
import math

import jax
import jax.numpy as jnp
import numpy as np
from jax import lax
from jax.experimental import pallas as pl
from jax.experimental.pallas import tpu as pltpu
from jax.sharding import PartitionSpec as P

NBR = 64
CELL = 8
AXES = ("gx", "gy", "gz")

coulomb_scale = 0.25
smearing = 1.0
highest = lax.Precision.HIGHEST


def round_bf16(x):
    return lax.reduce_precision(x, 8, 7)


def three_pieces(x):
    hi = round_bf16(x)
    mid = round_bf16(x - hi)
    lo = round_bf16(x - hi - mid)
    return hi, mid, lo


def cast_pieces(x, count):
    pieces = []
    for _ in range(count):
        piece = x.astype(jnp.bfloat16)
        pieces.append(piece)
        x = x - piece.astype(jnp.float32)
    return pieces


def silu(v):
    half = 0.5 * v
    return half + half * jnp.tanh(half)


def pair_kernel(
    cells,
    lengths,
    code_ref,
    ext_ref,
    own_ref,
    hidden_ref,
    wr_ref,
    rates_ref,
    w1_ref,
    w2_ref,
    wv_ref,
    wo_ref,
    out_ref,
    msg_ref,
    vec_ref,
    w1t_ref,
    w2t_ref,
):
    cells_x, cells_y, cells_z = cells
    f32, bf16 = jnp.float32, jnp.bfloat16
    slots = 8
    pairs = slots * NBR
    w1t_ref[...] = w1_ref[...].astype(f32).T.astype(bf16)
    w2t_ref[...] = w2_ref[...].astype(f32).T.astype(bf16)
    wr_rows = jnp.concatenate([wr_ref[...].astype(f32), jnp.zeros((8, 128), f32)], axis=1)
    zero_half = jnp.zeros((8, 128), f32)
    lane_slot = lax.broadcasted_iota(jnp.int32, (slots, pairs), 1) // NBR
    sel = jnp.where(lane_slot == lax.broadcasted_iota(jnp.int32, (slots, pairs), 0), 1.0, 0.0)
    tail = jnp.concatenate([sel, sel, sel, jnp.zeros((8, pairs), f32)], axis=0).astype(bf16)
    row_d = lax.broadcasted_iota(jnp.int32, (8, 1), 0)
    box = jnp.where(
        row_d == 0,
        float(lengths[0]),
        jnp.where(row_d == 1, float(lengths[1]), float(lengths[2])),
    )
    box_inv = 1.0 / box
    rates = rates_ref[...]

    def one_cell(c, carry):
        cz = c % cells_z
        cxy = c // cells_z
        cy = cxy % cells_y
        cx = cxy // cells_y
        row = pl.multiple_of(cz * 8, 8)
        here = pl.multiple_of(c * 8, 8)
        parts = []
        for dx in range(3):
            for dy in range(3):
                column = (cx + dx) * (cells_y + 2) + cy + dy
                parts.append(ext_ref[column, pl.ds(row, 24), :])
        mine = ext_ref[(cx + 1) * (cells_y + 2) + cy + 1, pl.ds(row + 8, 8), 128:]
        own = own_ref[pl.ds(here, 8), :]
        own_hi, own_mid, own_lo = [p.astype(f32) for p in cast_pieces(own, 3)]
        parts.append(wr_rows)
        parts.append(jnp.concatenate([own_hi, -mine], axis=1))
        parts.append(jnp.concatenate([own_mid, zero_half], axis=1))
        parts.append(jnp.concatenate([own_lo, zero_half], axis=1))
        parts.append(jnp.zeros((8, 256), f32))
        table = jnp.concatenate(parts, axis=0)
        sent_t = table[:, :128].T.astype(bf16)
        place_t = table[:, 128:].T[:32].astype(bf16)
        code = code_ref[c]
        which = code & 255
        live = jnp.where(code < 256, 1.0, 0.0)
        hot = jnp.where(
            lax.broadcasted_iota(jnp.int32, (216, pairs), 0) == which, 1.0, 0.0
        )
        hot_main = hot[:208].astype(bf16)
        hot_last = hot[208:]
        rhs_place = jnp.concatenate(
            [
                hot_main,
                jnp.concatenate([hot_last, jnp.zeros((8, pairs), f32)], axis=0).astype(bf16),
                tail,
            ],
            axis=0,
        )
        found = jnp.dot(place_t, rhs_place, preferred_element_type=f32)
        displace = found[0:8] + found[8:16] + found[16:24]
        displace = displace - box * jnp.floor(displace * box_inv + 0.5)
        scaled = displace * (1.0 / CELL)
        square = jnp.sum(scaled * scaled, axis=0, keepdims=True)
        basis = jnp.exp(-square * rates)
        rhs = jnp.concatenate(
            [hot_main, jnp.concatenate([hot_last, basis], axis=0).astype(bf16), tail], axis=0
        )
        pre = jnp.dot(sent_t, rhs, preferred_element_type=f32)
        latent = silu(pre).astype(bf16)
        second = silu(jnp.dot(w1t_ref[...], latent, preferred_element_type=f32)).astype(bf16)
        third = silu(jnp.dot(w2t_ref[...], second, preferred_element_type=f32)).astype(bf16)
        reach = scaled * live
        pieces = [p.astype(f32) for p in cast_pieces(reach, 3)]
        rows = [sel * live]
        for d in range(3):
            for piece in pieces:
                rows.append(sel * piece[d : d + 1])
        weights = jnp.concatenate(rows, axis=0).astype(bf16)
        sums = lax.dot_general(
            weights, third, (((1,), (1,)), ((), ())), preferred_element_type=f32
        )
        msg_ref[pl.ds(here, 8), :] = sums[0:8] * (1.0 / NBR)
        for d in range(3):
            base = 8 + 24 * d
            vec_ref[d, pl.ds(here, 8), :] = (
                sums[base : base + 8] + sums[base + 8 : base + 16] + sums[base + 16 : base + 24]
            )
        return carry

    lax.fori_loop(0, cells_x * cells_y * cells_z, one_cell, 0)
    wv = wv_ref[...].astype(f32)
    invariant = None
    for d in range(3):
        vector = jnp.dot(
            vec_ref[d], wv, precision=highest, preferred_element_type=f32
        ) * (1.0 / math.sqrt(NBR))
        part = vector * vector
        invariant = part if invariant is None else invariant + part
    update = (msg_ref[...] + invariant).astype(bf16)
    out_ref[...] = (
        hidden_ref[...].astype(f32)
        + jnp.dot(update, wo_ref[...], preferred_element_type=f32)
    ).astype(bf16)


def spline(distance):
    outer = jnp.maximum(2.0 - distance, 0.0)
    inner = jnp.maximum(1.0 - distance, 0.0)
    return (outer * outer * outer - 4.0 * (inner * inner * inner)) * (1.0 / 6.0)


def trig_basis(length):
    r = np.arange(length)
    rows = [np.cos(2 * np.pi * ((k * r) % length) / length) for k in range(length // 2 + 1)]
    rows += [np.sin(2 * np.pi * ((k * r) % length) / length) for k in range(1, length // 2)]
    modes = np.array(list(range(length // 2 + 1)) + list(range(1, length // 2)))
    return np.stack(rows), modes


def axis_terms(modes, length):
    wave = modes * (2.0 * np.pi / length)
    turn = np.exp(2j * np.pi * modes / length)
    modulus = np.abs(1 / 6 + 4 / 6 * turn + 1 / 6 * turn * turn) ** 2
    weight = np.where((modes == 0) | (2 * modes == length), 1.0, 2.0) / length
    return wave * wave, weight / modulus


def charge_kernel(
    sizes,
    lengths,
    window,
    screen,
    planes,
    atoms_ref,
    zrow_ref,
    krow_ref,
    kx_ref,
    by_ref,
    byt_ref,
    bx_ref,
    bxt_ref,
    out_ref,
    plane_ref,
    wave_ref,
):
    devices_x, devices_y, devices_z = sizes
    length_x, length_y, length_z = lengths
    grid_y = length_y // devices_y
    f32, bf16 = jnp.float32, jnp.bfloat16
    lanes = atoms_ref.shape[-1] * devices_z

    def load(gx, gy):
        base = (gx * devices_y + gy) * devices_z
        return jnp.concatenate([atoms_ref[base + i] for i in range(devices_z)], axis=1)

    def stencils(atoms, gy):
        ids_x = lax.broadcasted_iota(jnp.int32, (length_x, lanes), 0).astype(f32)
        off_x = jnp.abs(ids_x - atoms[0:1])
        rows_x = spline(jnp.minimum(off_x, length_x - off_x))
        start = (gy * grid_y - 1).astype(f32)
        ids_y = lax.broadcasted_iota(jnp.int32, (window, lanes), 0).astype(f32)
        rows_y = spline(jnp.abs(ids_y - (atoms[1:2] - start)))
        return rows_x, rows_y

    zrow = zrow_ref[my_index(sizes)]

    def spread(gx, gy):
        atoms = load(gx, gy)
        rows_x, rows_y = stencils(atoms, gy)
        place_z = atoms[2:3]
        whole = jnp.floor(place_z)
        f = place_z - whole
        sq = f * f
        cube = sq * f
        rem = 1.0 - f
        taps = [
            rem * rem * rem * (1.0 / 6.0),
            (3.0 * cube - 6.0 * sq + 4.0) * (1.0 / 6.0),
            (-3.0 * cube + 3.0 * sq + 3.0 * f + 1.0) * (1.0 / 6.0),
            cube * (1.0 / 6.0),
        ]
        turns = zrow[:, 0:1] * (whole - 1.0)
        turns = turns - length_z * jnp.floor(turns * (1.0 / length_z))
        angle = (turns - 0.5 * length_z) * (2.0 * math.pi / length_z)
        cos_a = -jnp.cos(angle)
        sin_a = -jnp.sin(angle)
        shift_c = zrow[:, 1:2]
        shift_s = zrow[:, 2:3]
        base_c = cos_a * shift_c + sin_a * shift_s
        base_s = sin_a * shift_c - cos_a * shift_s
        even = taps[0]
        odd = 0.0
        for t in range(1, 4):
            even = even + taps[t] * zrow[:, 2 + t : 3 + t]
            odd = odd + taps[t] * zrow[:, 5 + t : 6 + t]
        wave = base_c * even - base_s * odd
        wave_ref[gx * devices_y + gy] = wave
        scaled = wave * atoms[3:4]
        left = jnp.concatenate([rows_y * scaled[j : j + 1] for j in range(planes)], axis=0)
        left_hi = left.astype(bf16)
        left_lo = (left - left_hi.astype(f32)).astype(bf16)
        x_hi = rows_x.astype(bf16)
        x_lo = (rows_x - x_hi.astype(f32)).astype(bf16)
        res = lax.dot_general(
            jnp.concatenate([left_hi, left_lo], axis=0),
            jnp.concatenate([x_hi, x_lo], axis=0),
            (((1,), (1,)), ((), ())),
            preferred_element_type=f32,
        )
        half = planes * window
        res = res[:half] + res[half:]
        return res[:, :length_x] + res[:, length_x:]

    plane_ref[...] = jnp.zeros(plane_ref.shape, f32)

    def spread_group(g, carry):
        gy = g % devices_y
        total = spread(g // devices_y, gy)
        rows = pl.ds(pl.multiple_of(gy * window, 8), window)
        for j in range(planes):
            plane_ref[j, rows, :] += total[j * window : (j + 1) * window]
        return carry

    lax.fori_loop(0, devices_x * devices_y, spread_group, 0)

    def hdot(a, b):
        return jnp.dot(a, b, precision=highest, preferred_element_type=f32)

    along_y = jnp.concatenate([hdot(by_ref[...], plane_ref[j]) for j in range(planes)], axis=0)
    spectrum = hdot(along_y, bxt_ref[...])
    kcol = krow_ref[...]
    filtered = []
    for j in range(planes):
        q = kcol[:, 0:1] + zrow[j : j + 1, 9:10] + kx_ref[0:1, :]
        scale = kcol[:, 1:2] * zrow[j : j + 1, 10:11] * kx_ref[1:2, :]
        green = (coulomb_scale * 4.0 * math.pi) * jnp.exp(-0.5 * smearing * smearing * q)
        green = green * scale / (q + 1.0 / (screen * screen))
        green = jnp.where(q == 0.0, 0.0, green)
        filtered.append(spectrum[j * length_y : (j + 1) * length_y] * green)
    back = hdot(jnp.concatenate(filtered, axis=0), bx_ref[...])
    for j in range(planes):
        plane_ref[j] = hdot(byt_ref[...], back[j * length_y : (j + 1) * length_y])

    def sample_group(g, carry):
        gy = g % devices_y
        rows = pl.ds(pl.multiple_of(gy * window, 8), window)
        field = jnp.concatenate([plane_ref[j, rows, :] for j in range(planes)], axis=0)
        f_hi, f_mid = [p.astype(f32) for p in cast_pieces(field, 2)]
        field3 = jnp.concatenate([f_hi, f_mid, f_hi], axis=1).astype(bf16)
        atoms = load(g // devices_y, gy)
        rows_x, rows_y = stencils(atoms, gy)
        x_hi = rows_x.astype(bf16)
        x_lo = (rows_x - x_hi.astype(f32)).astype(bf16)
        values = jnp.dot(
            field3, jnp.concatenate([x_hi, x_hi, x_lo], axis=0), preferred_element_type=f32
        )
        wave = wave_ref[g]
        mixed = values[0:window] * wave[0:1]
        for j in range(1, planes):
            mixed = mixed + values[j * window : (j + 1) * window] * wave[j : j + 1]
        line = jnp.sum(mixed * rows_y, axis=0, keepdims=True)
        count = atoms_ref.shape[-1]
        for i in range(devices_z):
            out_ref[g * devices_z + i] = line[:, i * count : (i + 1) * count]
        return carry

    lax.fori_loop(0, devices_x * devices_y, sample_group, 0)


def coords_of(index, sizes):
    return (
        index // (sizes[1] * sizes[2]),
        (index // sizes[2]) % sizes[1],
        index % sizes[2],
    )


def my_index(sizes):
    gx, gy, gz = (lax.axis_index(a) for a in AXES)
    return (gx * sizes[1] + gy) * sizes[2] + gz


def gather_kernel(
    sizes, cells, atoms_ref, rows_ref, all_ref, ext_ref, asend, arecv, hsend, hrecv, local_sem
):
    devices = sizes[0] * sizes[1] * sizes[2]
    here = tuple(lax.axis_index(a) for a in AXES)
    me = my_index(sizes)
    copies = []
    for shift in range(27):
        step = (shift // 9 - 1, shift // 3 % 3 - 1, shift % 3 - 1)
        if step == (0, 0, 0):
            continue
        source, target, peer = [], [], []
        for axis in range(3):
            size = cells[axis]
            if step[axis] == 0:
                source.append(pl.ds(0, size))
                target.append(pl.ds(1, size))
                peer.append(here[axis])
            elif step[axis] > 0:
                source.append(pl.ds(size - 1, 1))
                target.append(pl.ds(0, 1))
                peer.append(lax.rem(here[axis] + 1, sizes[axis]))
            else:
                source.append(pl.ds(0, 1))
                target.append(pl.ds(size + 1, 1))
                peer.append(lax.rem(here[axis] + sizes[axis] - 1, sizes[axis]))
        copy = pltpu.make_async_remote_copy(
            src_ref=rows_ref.at[tuple(source)],
            dst_ref=ext_ref.at[tuple(target)],
            send_sem=hsend.at[shift],
            recv_sem=hrecv.at[shift],
            device_id=tuple(peer),
            device_id_type=pl.DeviceIdType.MESH,
        )
        copies.append(copy)

    def atom_copy(o):
        peer = lax.rem(me + o, devices)
        return pltpu.make_async_remote_copy(
            src_ref=atoms_ref,
            dst_ref=all_ref.at[me],
            send_sem=asend.at[o],
            recv_sem=arecv.at[o],
            device_id=coords_of(peer, sizes),
            device_id_type=pl.DeviceIdType.MESH,
        )

    def start(o, carry):
        atom_copy(o).start()
        return carry

    lax.fori_loop(1, devices, start, 0)
    for copy in copies:
        copy.start()
    inner = tuple(pl.ds(1, size) for size in cells)
    local = pltpu.make_async_copy(rows_ref, ext_ref.at[inner], local_sem.at[0])
    local.start()
    local_atoms = pltpu.make_async_copy(atoms_ref, all_ref.at[me], local_sem.at[1])
    local_atoms.start()
    local.wait()
    local_atoms.wait()

    def finish(o, carry):
        origin = lax.rem(me + devices - o, devices)
        pltpu.make_async_remote_copy(
            src_ref=atoms_ref,
            dst_ref=all_ref.at[origin],
            send_sem=asend.at[o],
            recv_sem=arecv.at[o],
            device_id=coords_of(origin, sizes),
            device_id_type=pl.DeviceIdType.MESH,
        ).wait()
        return carry

    lax.fori_loop(1, devices, finish, 0)
    for copy in copies:
        copy.wait()


def scatter_kernel(sizes, part_ref, out_ref, held_ref, send, recv):
    devices = sizes[0] * sizes[1] * sizes[2]
    me = my_index(sizes)

    def copy_to(o):
        peer = lax.rem(me + o, devices)
        return pltpu.make_async_remote_copy(
            src_ref=part_ref.at[peer],
            dst_ref=held_ref.at[o],
            send_sem=send.at[o],
            recv_sem=recv.at[o],
            device_id=coords_of(peer, sizes),
            device_id_type=pl.DeviceIdType.MESH,
        )

    def start(o, carry):
        copy_to(o).start()
        return carry

    lax.fori_loop(1, devices, start, 0)

    def finish(o, total):
        copy_to(o).wait()
        return total + held_ref[o]

    out_ref[...] = lax.fori_loop(1, devices, finish, part_ref[me])


def shards(
    features,
    positions,
    grid_anchor,
    species,
    neighbours,
    neighbour_count,
    w_self,
    w_neighbour,
    w_radial,
    radial_rates,
    w_pair1,
    w_pair2,
    w_vector,
    w_out,
    w_charge,
    species_charge,
):
    f32, bf16 = jnp.float32, jnp.bfloat16
    cells_x, cells_y, cells_z, slot_count, channels = features.shape
    cell_count = cells_x * cells_y * cells_z
    atom_count = cell_count * slot_count
    sizes = tuple(lax.axis_size(a) for a in AXES)
    devices = sizes[0] * sizes[1] * sizes[2]
    totals = (cells_x * sizes[0], cells_y * sizes[1], cells_z * sizes[2])
    lengths = tuple(t * CELL for t in totals)
    length_x, length_y, length_z = lengths
    screen = 2 * cells_y * CELL

    hidden = features.reshape(atom_count, channels)
    own = jnp.dot(hidden, w_self, preferred_element_type=f32)
    sent = jnp.dot(hidden, w_neighbour, preferred_element_type=f32).astype(bf16)
    species_rows = species.reshape(atom_count)
    kind_ids = jnp.arange(species_charge.shape[0], dtype=jnp.int32)
    base_charge = jnp.sum(
        jnp.where(species_rows[:, None] == kind_ids[None, :], species_charge[None, :], 0.0), axis=1
    )
    charge = base_charge + jnp.dot(hidden, w_charge, preferred_element_type=f32)
    place = positions.reshape(cell_count, 3, slot_count)
    place_cols = jnp.moveaxis(place, 1, 0).reshape(3, atom_count)
    atoms = jnp.concatenate([place_cols, charge[None]], axis=0)

    hi, mid, lo = three_pieces(jnp.moveaxis(place, 1, 2).reshape(atom_count, 3))
    gap = jnp.zeros((atom_count, 5), f32)
    place_rows = jnp.concatenate(
        [hi, gap, mid, gap, lo, gap, jnp.zeros((atom_count, channels - 24), f32)], axis=1
    ).astype(bf16)
    rows = jnp.concatenate([sent, place_rows], axis=1)
    rows = rows.reshape(cells_x, cells_y, cells_z, slot_count, 2 * channels)
    cells = (cells_x, cells_y, cells_z)
    vmem = pl.BlockSpec(memory_space=pltpu.VMEM)
    dma = pltpu.SemaphoreType.DMA
    atoms, ext = pl.pallas_call(
        functools.partial(gather_kernel, sizes, cells),
        out_shape=(
            jax.ShapeDtypeStruct((devices,) + atoms.shape, f32),
            jax.ShapeDtypeStruct(
                tuple(c + 2 for c in cells) + (slot_count, 2 * channels), bf16
            ),
        ),
        in_specs=[vmem] * 2,
        out_specs=(vmem, vmem),
        scratch_shapes=[dma((devices,)), dma((devices,)), dma((27,)), dma((27,)), dma((2,))],
        name="gather_atoms",
        compiler_params=pltpu.CompilerParams(has_side_effects=True),
    )(atoms, rows)
    ext = ext.astype(f32).reshape(
        (cells_x + 2) * (cells_y + 2), (cells_z + 2) * slot_count, 2 * channels
    )

    listed = neighbours.reshape(cells_x, cells_y, cells_z, slot_count * NBR)
    slot_ids = listed % slot_count
    cell_ids = listed // slot_count
    steps = []
    for axis, ids in enumerate(
        (cell_ids // (totals[2] * totals[1]), cell_ids // totals[2] % totals[1], cell_ids % totals[2])
    ):
        local = lax.broadcasted_iota(jnp.int32, listed.shape, axis)
        first = lax.axis_index(AXES[axis]) * (cells_x, cells_y, cells_z)[axis]
        steps.append((ids - first - local + 1 + totals[axis]) % totals[axis])
    code = ((steps[0] * 3 + steps[1]) * 3 + steps[2]) * slot_count + slot_ids
    counts = neighbour_count.reshape(cell_count, slot_count, 1)
    dead = jnp.arange(NBR, dtype=jnp.int32)[None, None, :] >= counts
    code = code.reshape(cell_count, slot_count, NBR) + jnp.where(dead, 256, 0)
    code = code.reshape(cell_count, 1, slot_count * NBR)

    vmem = pl.BlockSpec(memory_space=pltpu.VMEM)
    updated = pl.pallas_call(
        functools.partial(pair_kernel, (cells_x, cells_y, cells_z), lengths),
        out_shape=jax.ShapeDtypeStruct((atom_count, channels), bf16),
        in_specs=[vmem] * 10,
        out_specs=vmem,
        scratch_shapes=[
            pltpu.VMEM((atom_count, channels), f32),
            pltpu.VMEM((3, atom_count, channels), f32),
            pltpu.VMEM((channels, channels), bf16),
            pltpu.VMEM((channels, channels), bf16),
        ],
        name="pair_layer",
        cost_estimate=pl.CostEstimate(
            flops=2 * atom_count * NBR * channels * 512,
            bytes_accessed=4 * 1024 * 1024,
            transcendentals=3 * atom_count * NBR * channels,
        ),
    )(
        code,
        ext,
        own,
        hidden,
        w_radial,
        radial_rates.reshape(-1, 1),
        w_pair1,
        w_pair2,
        w_vector,
        w_out,
    )

    share = length_z // 2 // devices
    planes = 2 * share
    window = -(-(cells_y * CELL + 4) // 8) * 8
    all_modes = np.arange(length_z // 2)
    table_k = np.stack([all_modes, all_modes], axis=1)
    phase_c = np.stack([np.ones_like(all_modes), np.zeros_like(all_modes)], axis=1)
    table_k[0, 1] = length_z // 2
    phase_c[0, 1] = 1
    table_k = table_k.reshape(devices, planes)
    phase_c = phase_c.reshape(devices, planes).astype(np.float64)
    taps = [2 * np.pi * ((table_k * t) % length_z) / length_z for t in range(1, 4)]
    basis_x, modes_x = trig_basis(length_x)
    basis_y, modes_y = trig_basis(length_y)
    qx, sx = axis_terms(modes_x, length_x)
    qy, sy = axis_terms(modes_y, length_y)
    qz, sz = axis_terms(table_k, length_z)
    krow = np.stack([qy, sy], axis=1).astype(np.float32)
    zrow = np.stack(
        [table_k, phase_c, 1.0 - phase_c]
        + [np.cos(a) for a in taps]
        + [np.sin(a) for a in taps]
        + [qz, sz],
        axis=2,
    ).astype(np.float32)
    kx = np.stack([qx, sx]).astype(np.float32)
    grid_y = cells_y * CELL
    columns = np.concatenate(
        [(np.arange(window) + g * grid_y - 1) % length_y for g in range(sizes[1])]
    )
    by = basis_y[:, columns].astype(np.float32)
    bx = basis_x.astype(np.float32)
    partial = pl.pallas_call(
        functools.partial(charge_kernel, sizes, lengths, window, screen, planes),
        out_shape=jax.ShapeDtypeStruct((devices, 1, atom_count), f32),
        in_specs=[vmem] * 8,
        out_specs=vmem,
        scratch_shapes=[
            pltpu.VMEM((planes, sizes[1] * window, length_x), f32),
            pltpu.VMEM((sizes[0] * sizes[1], planes, sizes[2] * atom_count), f32),
        ],
        name="charge_solve",
        cost_estimate=pl.CostEstimate(
            flops=10**10, bytes_accessed=2 * 1024 * 1024, transcendentals=10**6
        ),
    )(
        atoms,
        jnp.asarray(zrow),
        jnp.asarray(krow),
        jnp.asarray(kx),
        jnp.asarray(by),
        jnp.asarray(np.ascontiguousarray(by.T)),
        jnp.asarray(bx),
        jnp.asarray(np.ascontiguousarray(bx.T)),
    )
    site_potential = pl.pallas_call(
        functools.partial(scatter_kernel, sizes),
        out_shape=jax.ShapeDtypeStruct((1, atom_count), f32),
        in_specs=[vmem],
        out_specs=vmem,
        scratch_shapes=[
            pltpu.VMEM((devices, 1, atom_count), f32),
            dma((devices,)),
            dma((devices,)),
        ],
        name="scatter_sum",
        compiler_params=pltpu.CompilerParams(has_side_effects=True),
    )(partial)
    return (
        updated.reshape(features.shape),
        site_potential.reshape(cells_x, cells_y, cells_z, slot_count),
    )


def solution(mesh):
    return jax.shard_map(
        shards,
        mesh=mesh,
        in_specs=(
            P("gx", "gy", "gz", None, None),
            P("gx", "gy", "gz", None),
            P("gx", "gy", "gz", None),
            P("gx", "gy", "gz", None),
            P("gx", "gy", "gz", None),
            P("gx", "gy", "gz", None),
            P(),
            P(),
            P(),
            P(),
            P(),
            P(),
            P(),
            P(),
            P(),
            P(),
        ),
        out_specs=(P("gx", "gy", "gz", None, None), P("gx", "gy", "gz", None)),
        check_vma=False,
    )
```

```python
import functools
import math

import jax
import jax.numpy as jnp
import numpy as np
from jax import lax
from jax.experimental import pallas as pl
from jax.experimental.pallas import tpu as pltpu
from jax.sharding import PartitionSpec as P

NBR = 64
CELL = 8
AXES = ("gx", "gy", "gz")

coulomb_scale = 0.25
smearing = 1.0
highest = lax.Precision.HIGHEST


def round_bf16(x):
    return lax.reduce_precision(x, 8, 7)


def three_pieces(x):
    hi = round_bf16(x)
    mid = round_bf16(x - hi)
    lo = round_bf16(x - hi - mid)
    return hi, mid, lo


def cast_pieces(x, count):
    pieces = []
    for _ in range(count):
        piece = x.astype(jnp.bfloat16)
        pieces.append(piece)
        x = x - piece.astype(jnp.float32)
    return pieces


def silu(v):
    half = 0.5 * v
    return half + half * jnp.tanh(half)


def pair_kernel(
    cells,
    lengths,
    code_ref,
    ext_ref,
    own_ref,
    hidden_ref,
    wr_ref,
    rates_ref,
    w1_ref,
    w2_ref,
    wv_ref,
    wo_ref,
    out_ref,
    msg_ref,
    vec_ref,
    w1t_ref,
    w2t_ref,
):
    cells_x, cells_y, cells_z = cells
    f32, bf16 = jnp.float32, jnp.bfloat16
    slots = 8
    pairs = slots * NBR
    w1t_ref[...] = w1_ref[...].astype(f32).T.astype(bf16)
    w2t_ref[...] = w2_ref[...].astype(f32).T.astype(bf16)
    wr_rows = jnp.concatenate([wr_ref[...].astype(f32), jnp.zeros((8, 128), f32)], axis=1)
    zero_half = jnp.zeros((8, 128), f32)
    lane_slot = lax.broadcasted_iota(jnp.int32, (slots, pairs), 1) // NBR
    sel = jnp.where(lane_slot == lax.broadcasted_iota(jnp.int32, (slots, pairs), 0), 1.0, 0.0)
    tail = jnp.concatenate([sel, sel, sel, jnp.zeros((8, pairs), f32)], axis=0).astype(bf16)
    row_d = lax.broadcasted_iota(jnp.int32, (8, 1), 0)
    box = jnp.where(
        row_d == 0,
        float(lengths[0]),
        jnp.where(row_d == 1, float(lengths[1]), float(lengths[2])),
    )
    box_inv = 1.0 / box
    rates = rates_ref[...]

    def one_cell(c, carry):
        cz = c % cells_z
        cxy = c // cells_z
        cy = cxy % cells_y
        cx = cxy // cells_y
        row = pl.multiple_of(cz * 8, 8)
        here = pl.multiple_of(c * 8, 8)
        parts = []
        for dx in range(3):
            for dy in range(3):
                column = (cx + dx) * (cells_y + 2) + cy + dy
                parts.append(ext_ref[column, pl.ds(row, 24), :])
        mine = ext_ref[(cx + 1) * (cells_y + 2) + cy + 1, pl.ds(row + 8, 8), 128:]
        own = own_ref[pl.ds(here, 8), :]
        own_hi, own_mid, own_lo = [p.astype(f32) for p in cast_pieces(own, 3)]
        parts.append(wr_rows)
        parts.append(jnp.concatenate([own_hi, -mine], axis=1))
        parts.append(jnp.concatenate([own_mid, zero_half], axis=1))
        parts.append(jnp.concatenate([own_lo, zero_half], axis=1))
        parts.append(jnp.zeros((8, 256), f32))
        table = jnp.concatenate(parts, axis=0)
        sent_t = table[:, :128].T.astype(bf16)
        place_t = table[:, 128:].T[:32].astype(bf16)
        code = code_ref[c]
        which = code & 255
        live = jnp.where(code < 256, 1.0, 0.0)
        hot = jnp.where(
            lax.broadcasted_iota(jnp.int32, (216, pairs), 0) == which, 1.0, 0.0
        )
        hot_main = hot[:208].astype(bf16)
        hot_last = hot[208:]
        rhs_place = jnp.concatenate(
            [
                hot_main,
                jnp.concatenate([hot_last, jnp.zeros((8, pairs), f32)], axis=0).astype(bf16),
                tail,
            ],
            axis=0,
        )
        found = jnp.dot(place_t, rhs_place, preferred_element_type=f32)
        displace = found[0:8] + found[8:16] + found[16:24]
        displace = displace - box * jnp.floor(displace * box_inv + 0.5)
        scaled = displace * (1.0 / CELL)
        square = jnp.sum(scaled * scaled, axis=0, keepdims=True)
        basis = jnp.exp(-square * rates)
        rhs = jnp.concatenate(
            [hot_main, jnp.concatenate([hot_last, basis], axis=0).astype(bf16), tail], axis=0
        )
        pre = jnp.dot(sent_t, rhs, preferred_element_type=f32)
        latent = silu(pre).astype(bf16)
        second = silu(jnp.dot(w1t_ref[...], latent, preferred_element_type=f32)).astype(bf16)
        third = silu(jnp.dot(w2t_ref[...], second, preferred_element_type=f32)).astype(bf16)
        reach = scaled * live
        pieces = [p.astype(f32) for p in cast_pieces(reach, 3)]
        rows = [sel * live]
        for d in range(3):
            for piece in pieces:
                rows.append(sel * piece[d : d + 1])
        weights = jnp.concatenate(rows, axis=0).astype(bf16)
        sums = lax.dot_general(
            weights, third, (((1,), (1,)), ((), ())), preferred_element_type=f32
        )
        msg_ref[pl.ds(here, 8), :] = sums[0:8] * (1.0 / NBR)
        for d in range(3):
            base = 8 + 24 * d
            vec_ref[d, pl.ds(here, 8), :] = (
                sums[base : base + 8] + sums[base + 8 : base + 16] + sums[base + 16 : base + 24]
            )
        return carry

    lax.fori_loop(0, cells_x * cells_y * cells_z, one_cell, 0, unroll=8)
    wv = wv_ref[...].astype(f32)
    invariant = None
    for d in range(3):
        vector = jnp.dot(
            vec_ref[d], wv, precision=highest, preferred_element_type=f32
        ) * (1.0 / math.sqrt(NBR))
        part = vector * vector
        invariant = part if invariant is None else invariant + part
    update = (msg_ref[...] + invariant).astype(bf16)
    out_ref[...] = (
        hidden_ref[...].astype(f32)
        + jnp.dot(update, wo_ref[...], preferred_element_type=f32)
    ).astype(bf16)


def spline(distance):
    outer = jnp.maximum(2.0 - distance, 0.0)
    inner = jnp.maximum(1.0 - distance, 0.0)
    return (outer * outer * outer - 4.0 * (inner * inner * inner)) * (1.0 / 6.0)


def trig_basis(length):
    r = np.arange(length)
    rows = [np.cos(2 * np.pi * ((k * r) % length) / length) for k in range(length // 2 + 1)]
    rows += [np.sin(2 * np.pi * ((k * r) % length) / length) for k in range(1, length // 2)]
    modes = np.array(list(range(length // 2 + 1)) + list(range(1, length // 2)))
    return np.stack(rows), modes


def axis_terms(modes, length):
    wave = modes * (2.0 * np.pi / length)
    turn = np.exp(2j * np.pi * modes / length)
    modulus = np.abs(1 / 6 + 4 / 6 * turn + 1 / 6 * turn * turn) ** 2
    weight = np.where((modes == 0) | (2 * modes == length), 1.0, 2.0) / length
    return wave * wave, weight / modulus


def charge_kernel(
    sizes,
    lengths,
    window,
    screen,
    planes,
    atoms_ref,
    zrow_ref,
    krow_ref,
    kx_ref,
    by_ref,
    byt_ref,
    bx_ref,
    bxt_ref,
    out_ref,
    plane_ref,
    wave_ref,
):
    devices_x, devices_y, devices_z = sizes
    length_x, length_y, length_z = lengths
    grid_y = length_y // devices_y
    f32, bf16 = jnp.float32, jnp.bfloat16
    lanes = atoms_ref.shape[-1] * devices_z

    def load(gx, gy):
        base = (gx * devices_y + gy) * devices_z
        return jnp.concatenate([atoms_ref[base + i] for i in range(devices_z)], axis=1)

    def stencils(atoms, gy):
        ids_x = lax.broadcasted_iota(jnp.int32, (length_x, lanes), 0).astype(f32)
        off_x = jnp.abs(ids_x - atoms[0:1])
        rows_x = spline(jnp.minimum(off_x, length_x - off_x))
        start = (gy * grid_y - 1).astype(f32)
        ids_y = lax.broadcasted_iota(jnp.int32, (window, lanes), 0).astype(f32)
        rows_y = spline(jnp.abs(ids_y - (atoms[1:2] - start)))
        return rows_x, rows_y

    zrow = zrow_ref[my_index(sizes)]

    def spread(gx, gy):
        atoms = load(gx, gy)
        rows_x, rows_y = stencils(atoms, gy)
        place_z = atoms[2:3]
        whole = jnp.floor(place_z)
        f = place_z - whole
        sq = f * f
        cube = sq * f
        rem = 1.0 - f
        taps = [
            rem * rem * rem * (1.0 / 6.0),
            (3.0 * cube - 6.0 * sq + 4.0) * (1.0 / 6.0),
            (-3.0 * cube + 3.0 * sq + 3.0 * f + 1.0) * (1.0 / 6.0),
            cube * (1.0 / 6.0),
        ]
        turns = zrow[:, 0:1] * (whole - 1.0)
        turns = turns - length_z * jnp.floor(turns * (1.0 / length_z))
        angle = (turns - 0.5 * length_z) * (2.0 * math.pi / length_z)
        cos_a = -jnp.cos(angle)
        sin_a = -jnp.sin(angle)
        shift_c = zrow[:, 1:2]
        shift_s = zrow[:, 2:3]
        base_c = cos_a * shift_c + sin_a * shift_s
        base_s = sin_a * shift_c - cos_a * shift_s
        even = taps[0]
        odd = 0.0
        for t in range(1, 4):
            even = even + taps[t] * zrow[:, 2 + t : 3 + t]
            odd = odd + taps[t] * zrow[:, 5 + t : 6 + t]
        wave = base_c * even - base_s * odd
        wave_ref[gx * devices_y + gy] = wave
        scaled = wave * atoms[3:4]
        left = jnp.concatenate([rows_y * scaled[j : j + 1] for j in range(planes)], axis=0)
        left_hi = left.astype(bf16)
        left_lo = (left - left_hi.astype(f32)).astype(bf16)
        x_hi = rows_x.astype(bf16)
        x_lo = (rows_x - x_hi.astype(f32)).astype(bf16)
        res = lax.dot_general(
            jnp.concatenate([left_hi, left_lo], axis=0),
            jnp.concatenate([x_hi, x_lo], axis=0),
            (((1,), (1,)), ((), ())),
            preferred_element_type=f32,
        )
        half = planes * window
        res = res[:half] + res[half:]
        return res[:, :length_x] + res[:, length_x:]

    plane_ref[...] = jnp.zeros(plane_ref.shape, f32)

    def spread_group(g, carry):
        gy = g % devices_y
        total = spread(g // devices_y, gy)
        rows = pl.ds(pl.multiple_of(gy * window, 8), window)
        for j in range(planes):
            plane_ref[j, rows, :] += total[j * window : (j + 1) * window]
        return carry

    lax.fori_loop(0, devices_x * devices_y, spread_group, 0, unroll=2)

    def hdot(a, b):
        return jnp.dot(a, b, precision=highest, preferred_element_type=f32)

    along_y = jnp.concatenate([hdot(by_ref[...], plane_ref[j]) for j in range(planes)], axis=0)
    spectrum = hdot(along_y, bxt_ref[...])
    kcol = krow_ref[...]
    filtered = []
    for j in range(planes):
        q = kcol[:, 0:1] + zrow[j : j + 1, 9:10] + kx_ref[0:1, :]
        scale = kcol[:, 1:2] * zrow[j : j + 1, 10:11] * kx_ref[1:2, :]
        green = (coulomb_scale * 4.0 * math.pi) * jnp.exp(-0.5 * smearing * smearing * q)
        green = green * scale / (q + 1.0 / (screen * screen))
        green = jnp.where(q == 0.0, 0.0, green)
        filtered.append(spectrum[j * length_y : (j + 1) * length_y] * green)
    back = hdot(jnp.concatenate(filtered, axis=0), bx_ref[...])
    for j in range(planes):
        plane_ref[j] = hdot(byt_ref[...], back[j * length_y : (j + 1) * length_y])

    def sample_group(g, carry):
        gy = g % devices_y
        rows = pl.ds(pl.multiple_of(gy * window, 8), window)
        field = jnp.concatenate([plane_ref[j, rows, :] for j in range(planes)], axis=0)
        f_hi, f_mid = [p.astype(f32) for p in cast_pieces(field, 2)]
        field3 = jnp.concatenate([f_hi, f_mid, f_hi], axis=1).astype(bf16)
        atoms = load(g // devices_y, gy)
        rows_x, rows_y = stencils(atoms, gy)
        x_hi = rows_x.astype(bf16)
        x_lo = (rows_x - x_hi.astype(f32)).astype(bf16)
        values = jnp.dot(
            field3, jnp.concatenate([x_hi, x_hi, x_lo], axis=0), preferred_element_type=f32
        )
        wave = wave_ref[g]
        mixed = values[0:window] * wave[0:1]
        for j in range(1, planes):
            mixed = mixed + values[j * window : (j + 1) * window] * wave[j : j + 1]
        line = jnp.sum(mixed * rows_y, axis=0, keepdims=True)
        count = atoms_ref.shape[-1]
        for i in range(devices_z):
            out_ref[g * devices_z + i] = line[:, i * count : (i + 1) * count]
        return carry

    lax.fori_loop(0, devices_x * devices_y, sample_group, 0, unroll=2)


def coords_of(index, sizes):
    return (
        index // (sizes[1] * sizes[2]),
        (index // sizes[2]) % sizes[1],
        index % sizes[2],
    )


def my_index(sizes):
    gx, gy, gz = (lax.axis_index(a) for a in AXES)
    return (gx * sizes[1] + gy) * sizes[2] + gz


def gather_kernel(
    sizes, cells, atoms_ref, rows_ref, all_ref, ext_ref, asend, arecv, hsend, hrecv, local_sem
):
    devices = sizes[0] * sizes[1] * sizes[2]
    here = tuple(lax.axis_index(a) for a in AXES)
    me = my_index(sizes)
    copies = []
    for shift in range(27):
        step = (shift // 9 - 1, shift // 3 % 3 - 1, shift % 3 - 1)
        if step == (0, 0, 0):
            continue
        source, target, peer = [], [], []
        for axis in range(3):
            size = cells[axis]
            if step[axis] == 0:
                source.append(pl.ds(0, size))
                target.append(pl.ds(1, size))
                peer.append(here[axis])
            elif step[axis] > 0:
                source.append(pl.ds(size - 1, 1))
                target.append(pl.ds(0, 1))
                peer.append(lax.rem(here[axis] + 1, sizes[axis]))
            else:
                source.append(pl.ds(0, 1))
                target.append(pl.ds(size + 1, 1))
                peer.append(lax.rem(here[axis] + sizes[axis] - 1, sizes[axis]))
        copy = pltpu.make_async_remote_copy(
            src_ref=rows_ref.at[tuple(source)],
            dst_ref=ext_ref.at[tuple(target)],
            send_sem=hsend.at[shift],
            recv_sem=hrecv.at[shift],
            device_id=tuple(peer),
            device_id_type=pl.DeviceIdType.MESH,
        )
        copies.append(copy)

    def atom_copy(o):
        peer = lax.rem(me + o, devices)
        return pltpu.make_async_remote_copy(
            src_ref=atoms_ref,
            dst_ref=all_ref.at[me],
            send_sem=asend.at[o],
            recv_sem=arecv.at[o],
            device_id=coords_of(peer, sizes),
            device_id_type=pl.DeviceIdType.MESH,
        )

    def start(o, carry):
        atom_copy(o).start()
        return carry

    lax.fori_loop(1, devices, start, 0)
    for copy in copies:
        copy.start()
    inner = tuple(pl.ds(1, size) for size in cells)
    local = pltpu.make_async_copy(rows_ref, ext_ref.at[inner], local_sem.at[0])
    local.start()
    local_atoms = pltpu.make_async_copy(atoms_ref, all_ref.at[me], local_sem.at[1])
    local_atoms.start()
    local.wait()
    local_atoms.wait()

    def finish(o, carry):
        origin = lax.rem(me + devices - o, devices)
        pltpu.make_async_remote_copy(
            src_ref=atoms_ref,
            dst_ref=all_ref.at[origin],
            send_sem=asend.at[o],
            recv_sem=arecv.at[o],
            device_id=coords_of(origin, sizes),
            device_id_type=pl.DeviceIdType.MESH,
        ).wait()
        return carry

    lax.fori_loop(1, devices, finish, 0)
    for copy in copies:
        copy.wait()


def scatter_kernel(sizes, part_ref, out_ref, held_ref, send, recv):
    devices = sizes[0] * sizes[1] * sizes[2]
    me = my_index(sizes)

    def copy_to(o):
        peer = lax.rem(me + o, devices)
        return pltpu.make_async_remote_copy(
            src_ref=part_ref.at[peer],
            dst_ref=held_ref.at[o],
            send_sem=send.at[o],
            recv_sem=recv.at[o],
            device_id=coords_of(peer, sizes),
            device_id_type=pl.DeviceIdType.MESH,
        )

    def start(o, carry):
        copy_to(o).start()
        return carry

    lax.fori_loop(1, devices, start, 0)

    def finish(o, total):
        copy_to(o).wait()
        return total + held_ref[o]

    out_ref[...] = lax.fori_loop(1, devices, finish, part_ref[me])


def shards(
    features,
    positions,
    grid_anchor,
    species,
    neighbours,
    neighbour_count,
    w_self,
    w_neighbour,
    w_radial,
    radial_rates,
    w_pair1,
    w_pair2,
    w_vector,
    w_out,
    w_charge,
    species_charge,
):
    f32, bf16 = jnp.float32, jnp.bfloat16
    cells_x, cells_y, cells_z, slot_count, channels = features.shape
    cell_count = cells_x * cells_y * cells_z
    atom_count = cell_count * slot_count
    sizes = tuple(lax.axis_size(a) for a in AXES)
    devices = sizes[0] * sizes[1] * sizes[2]
    totals = (cells_x * sizes[0], cells_y * sizes[1], cells_z * sizes[2])
    lengths = tuple(t * CELL for t in totals)
    length_x, length_y, length_z = lengths
    screen = 2 * cells_y * CELL

    hidden = features.reshape(atom_count, channels)
    own = jnp.dot(hidden, w_self, preferred_element_type=f32)
    sent = jnp.dot(hidden, w_neighbour, preferred_element_type=f32).astype(bf16)
    species_rows = species.reshape(atom_count)
    kind_ids = jnp.arange(species_charge.shape[0], dtype=jnp.int32)
    base_charge = jnp.sum(
        jnp.where(species_rows[:, None] == kind_ids[None, :], species_charge[None, :], 0.0), axis=1
    )
    charge = base_charge + jnp.dot(hidden, w_charge, preferred_element_type=f32)
    place = positions.reshape(cell_count, 3, slot_count)
    place_cols = jnp.moveaxis(place, 1, 0).reshape(3, atom_count)
    atoms = jnp.concatenate([place_cols, charge[None]], axis=0)

    hi, mid, lo = three_pieces(jnp.moveaxis(place, 1, 2).reshape(atom_count, 3))
    gap = jnp.zeros((atom_count, 5), f32)
    place_rows = jnp.concatenate(
        [hi, gap, mid, gap, lo, gap, jnp.zeros((atom_count, channels - 24), f32)], axis=1
    ).astype(bf16)
    rows = jnp.concatenate([sent, place_rows], axis=1)
    rows = rows.reshape(cells_x, cells_y, cells_z, slot_count, 2 * channels)
    cells = (cells_x, cells_y, cells_z)
    vmem = pl.BlockSpec(memory_space=pltpu.VMEM)
    dma = pltpu.SemaphoreType.DMA
    atoms, ext = pl.pallas_call(
        functools.partial(gather_kernel, sizes, cells),
        out_shape=(
            jax.ShapeDtypeStruct((devices,) + atoms.shape, f32),
            jax.ShapeDtypeStruct(
                tuple(c + 2 for c in cells) + (slot_count, 2 * channels), bf16
            ),
        ),
        in_specs=[vmem] * 2,
        out_specs=(vmem, vmem),
        scratch_shapes=[dma((devices,)), dma((devices,)), dma((27,)), dma((27,)), dma((2,))],
        name="gather_atoms",
        compiler_params=pltpu.CompilerParams(has_side_effects=True),
    )(atoms, rows)
    ext = ext.astype(f32).reshape(
        (cells_x + 2) * (cells_y + 2), (cells_z + 2) * slot_count, 2 * channels
    )

    listed = neighbours.reshape(cells_x, cells_y, cells_z, slot_count * NBR)
    slot_ids = listed % slot_count
    cell_ids = listed // slot_count
    steps = []
    for axis, ids in enumerate(
        (cell_ids // (totals[2] * totals[1]), cell_ids // totals[2] % totals[1], cell_ids % totals[2])
    ):
        local = lax.broadcasted_iota(jnp.int32, listed.shape, axis)
        first = lax.axis_index(AXES[axis]) * (cells_x, cells_y, cells_z)[axis]
        steps.append((ids - first - local + 1 + totals[axis]) % totals[axis])
    code = ((steps[0] * 3 + steps[1]) * 3 + steps[2]) * slot_count + slot_ids
    counts = neighbour_count.reshape(cell_count, slot_count, 1)
    dead = jnp.arange(NBR, dtype=jnp.int32)[None, None, :] >= counts
    code = code.reshape(cell_count, slot_count, NBR) + jnp.where(dead, 256, 0)
    code = code.reshape(cell_count, 1, slot_count * NBR)

    vmem = pl.BlockSpec(memory_space=pltpu.VMEM)
    updated = pl.pallas_call(
        functools.partial(pair_kernel, (cells_x, cells_y, cells_z), lengths),
        out_shape=jax.ShapeDtypeStruct((atom_count, channels), bf16),
        in_specs=[vmem] * 10,
        out_specs=vmem,
        scratch_shapes=[
            pltpu.VMEM((atom_count, channels), f32),
            pltpu.VMEM((3, atom_count, channels), f32),
            pltpu.VMEM((channels, channels), bf16),
            pltpu.VMEM((channels, channels), bf16),
        ],
        name="pair_layer",
        cost_estimate=pl.CostEstimate(
            flops=2 * atom_count * NBR * channels * 512,
            bytes_accessed=4 * 1024 * 1024,
            transcendentals=3 * atom_count * NBR * channels,
        ),
    )(
        code,
        ext,
        own,
        hidden,
        w_radial,
        radial_rates.reshape(-1, 1),
        w_pair1,
        w_pair2,
        w_vector,
        w_out,
    )

    share = length_z // 2 // devices
    planes = 2 * share
    window = -(-(cells_y * CELL + 4) // 8) * 8
    all_modes = np.arange(length_z // 2)
    table_k = np.stack([all_modes, all_modes], axis=1)
    phase_c = np.stack([np.ones_like(all_modes), np.zeros_like(all_modes)], axis=1)
    table_k[0, 1] = length_z // 2
    phase_c[0, 1] = 1
    table_k = table_k.reshape(devices, planes)
    phase_c = phase_c.reshape(devices, planes).astype(np.float64)
    taps = [2 * np.pi * ((table_k * t) % length_z) / length_z for t in range(1, 4)]
    basis_x, modes_x = trig_basis(length_x)
    basis_y, modes_y = trig_basis(length_y)
    qx, sx = axis_terms(modes_x, length_x)
    qy, sy = axis_terms(modes_y, length_y)
    qz, sz = axis_terms(table_k, length_z)
    krow = np.stack([qy, sy], axis=1).astype(np.float32)
    zrow = np.stack(
        [table_k, phase_c, 1.0 - phase_c]
        + [np.cos(a) for a in taps]
        + [np.sin(a) for a in taps]
        + [qz, sz],
        axis=2,
    ).astype(np.float32)
    kx = np.stack([qx, sx]).astype(np.float32)
    grid_y = cells_y * CELL
    columns = np.concatenate(
        [(np.arange(window) + g * grid_y - 1) % length_y for g in range(sizes[1])]
    )
    by = basis_y[:, columns].astype(np.float32)
    bx = basis_x.astype(np.float32)
    partial = pl.pallas_call(
        functools.partial(charge_kernel, sizes, lengths, window, screen, planes),
        out_shape=jax.ShapeDtypeStruct((devices, 1, atom_count), f32),
        in_specs=[vmem] * 8,
        out_specs=vmem,
        scratch_shapes=[
            pltpu.VMEM((planes, sizes[1] * window, length_x), f32),
            pltpu.VMEM((sizes[0] * sizes[1], planes, sizes[2] * atom_count), f32),
        ],
        name="charge_solve",
        cost_estimate=pl.CostEstimate(
            flops=10**10, bytes_accessed=2 * 1024 * 1024, transcendentals=10**6
        ),
    )(
        atoms,
        jnp.asarray(zrow),
        jnp.asarray(krow),
        jnp.asarray(kx),
        jnp.asarray(by),
        jnp.asarray(np.ascontiguousarray(by.T)),
        jnp.asarray(bx),
        jnp.asarray(np.ascontiguousarray(bx.T)),
    )
    site_potential = pl.pallas_call(
        functools.partial(scatter_kernel, sizes),
        out_shape=jax.ShapeDtypeStruct((1, atom_count), f32),
        in_specs=[vmem],
        out_specs=vmem,
        scratch_shapes=[
            pltpu.VMEM((devices, 1, atom_count), f32),
            dma((devices,)),
            dma((devices,)),
        ],
        name="scatter_sum",
        compiler_params=pltpu.CompilerParams(has_side_effects=True),
    )(partial)
    return (
        updated.reshape(features.shape),
        site_potential.reshape(cells_x, cells_y, cells_z, slot_count),
    )


def solution(mesh):
    return jax.shard_map(
        shards,
        mesh=mesh,
        in_specs=(
            P("gx", "gy", "gz", None, None),
            P("gx", "gy", "gz", None),
            P("gx", "gy", "gz", None),
            P("gx", "gy", "gz", None),
            P("gx", "gy", "gz", None),
            P("gx", "gy", "gz", None),
            P(),
            P(),
            P(),
            P(),
            P(),
            P(),
            P(),
            P(),
            P(),
            P(),
        ),
        out_specs=(P("gx", "gy", "gz", None, None), P("gx", "gy", "gz", None)),
        check_vma=False,
    )
```
